128 devices in a mesh: gx: 16 (over y, x), gy: 8 (over z, core).
Axes of the slice: x: 4, y: 4, z: 4, core: 2. Of those that a mesh axis runs over, the one named last changes fastest.
Arguments:
- basis: float32 [32, 256, 128, 256], P(None, 'gx', 'gy'), may hold values from -0.09375 to 0.09375
- reaction: float32 [256, 128, 256], P('gx', 'gy'), may hold values from 0.5 to 4
Outputs:
- extended: float32 [32, 256, 128, 256], P(None, 'gx', 'gy')
- coarse: float32 [128, 5, 32, 32], replicated
The draws below stay inside these ranges and needn't reach their ends.
All inputs are finite; a program needn't handle non-finite values.
Results may differ from the reference program's by a relative error of at most 0.000071.
Values sent between devices are 32-bit elements; how exact they have to be, the bound alone decides.
No kernel may reach another device: no remote copies, remote signals or barrier semaphores. Data moves between devices by JAX's collectives and lax.ppermute only.
A program may use at most 128 MiB of HBM per device.

```python
import math
import jax
import jax.numpy as jnp
from jax import lax

K = 32
SWEEPS = 4
CX = 16
CY = 16
CZ = 256
NX = 256
NY = 128
N_GX = 16
N_GY = 8


def level_of(rng, extent, shards, smallest, high):
    factor_of, own = 1.0, jax.random.fold_in(rng, 6)
    for axis_at, blocks in shards:
        draws = jnp.exp(jax.random.uniform(jax.random.fold_in(own, axis_at), (blocks,), jnp.float32, smallest / len(shards), high / len(shards)))
        factor_of = factor_of * jnp.repeat(draws, extent[axis_at] // blocks).reshape([-1 if axis == axis_at else 1 for axis in range(len(extent))])
    return factor_of


def centred(rng, extent, width, limit, shards=(), dtype=jnp.bfloat16):
    loudness = level_of(rng, extent, shards, -0.22, 0.18) if shards else 1.0
    result = jax.random.normal(rng, extent, jnp.float32) * width * loudness
    return jnp.minimum(jnp.maximum(result, -limit), limit).astype(dtype)


def setup_inputs(seed: int = 0) -> dict:
    keys = jax.random.split(jax.random.key(seed), 3)
    basis = centred(keys[0], (K, NX, NY, CZ), (CY * CZ) ** -0.5, 0.09375, ((1, 16), (2, 8)), jnp.float32)
    reaction = jnp.clip(jnp.exp(math.log(4.0) - 2.0794415 * jax.random.uniform(keys[1], (NX, NY, CZ), jnp.float32) ** level_of(keys[1], (NX, NY, CZ), ((0, 16), (1, 8)), -0.2, 0.2)), 0.5, 4.0)
    return dict(basis=basis, reaction=reaction)


OMEGA = 0.8


def stencil(field, coef):
    padded = jnp.pad(field, ((0, 0), (1, 1), (1, 1), (1, 1)))
    beside = padded[:, 2:, 1:-1, 1:-1] + padded[:, :-2, 1:-1, 1:-1]
    beside = beside + padded[:, 1:-1, 2:, 1:-1] + padded[:, 1:-1, :-2, 1:-1]
    beside = beside + padded[:, 1:-1, 1:-1, 2:] + padded[:, 1:-1, 1:-1, :-2]
    return (6.0 + coef) * field - beside


def extend_one(pair):
    phi, coef = pair
    kk, cx, cy, cz = phi.shape
    xpos = lax.broadcasted_iota(jnp.int32, (cx, cy, cz), 0)
    ypos = lax.broadcasted_iota(jnp.int32, (cx, cy, cz), 1)
    inner = (xpos >= 1) & (xpos <= cx - 2) & (ypos >= 1) & (ypos <= cy - 2)
    for sweep in range(SWEEPS):
        update = OMEGA * stencil(phi, coef) / (6.0 + coef)
        phi = phi - jnp.where(inner[None], update, jnp.float32(0.0))
    applied = stencil(phi, coef)
    diag = jnp.dot(phi.reshape(kk, -1), applied.reshape(kk, -1).T,
                   precision=lax.Precision.HIGHEST, preferred_element_type=jnp.float32)
    return phi, diag


def couple(own, other):
    return -jnp.einsum("iabyz,jabyz->abij", own, other, precision=lax.Precision.HIGHEST)


def reference(basis, reaction):
    gxn, gyn = N_GX, N_GY
    blocked = basis.reshape(K, gxn, CX, gyn, CY, CZ)
    subs = blocked.transpose(1, 3, 0, 2, 4, 5).reshape(gxn * gyn, K, CX, CY, CZ)
    coefs = reaction.reshape(gxn, CX, gyn, CY, CZ).transpose(0, 2, 1, 3, 4).reshape(gxn * gyn, CX, CY, CZ)
    phis, diags = lax.map(extend_one, (subs, coefs))
    extended = phis.reshape(gxn, gyn, K, CX, CY, CZ).transpose(2, 0, 3, 1, 4, 5).reshape(K, gxn * CX, gyn * CY, CZ)
    low_x = blocked[:, :, 0]
    high_x = blocked[:, :, CX - 1]
    zero_x = jnp.zeros_like(low_x[:, :1])
    minus_x = couple(low_x, jnp.concatenate([zero_x, high_x[:, :-1]], axis=1))
    plus_x = couple(high_x, jnp.concatenate([low_x[:, 1:], zero_x], axis=1))
    low_y = blocked[:, :, :, :, 0].transpose(0, 1, 3, 2, 4)
    high_y = blocked[:, :, :, :, CY - 1].transpose(0, 1, 3, 2, 4)
    zero_y = jnp.zeros_like(low_y[:, :, :1])
    minus_y = couple(low_y, jnp.concatenate([zero_y, high_y[:, :, :-1]], axis=2))
    plus_y = couple(high_y, jnp.concatenate([low_y[:, :, 1:], zero_y], axis=2))
    count = gxn * gyn
    coarse = jnp.stack([diags, minus_x.reshape(count, K, K), plus_x.reshape(count, K, K),
                        minus_y.reshape(count, K, K), plus_y.reshape(count, K, K)], axis=1)
    return extended, coarse
```

```python
import functools

import jax
import jax.numpy as jnp
from jax import lax
from jax.experimental import pallas as pl
from jax.experimental.pallas import tpu as pltpu
from jax.sharding import Mesh, PartitionSpec as P

K = 32
ROWS = 512
PITCH = 516
FPITCH = 36
OMEGA = 0.8
SWEEPS = 4
F32 = jnp.float32
BF16 = jnp.bfloat16
ANY = pl.BlockSpec(memory_space=pl.ANY)
VM = pl.BlockSpec(memory_space=pltpu.VMEM)


def rows_of(block):
    n = block.shape[0]
    return block.reshape(n, 16, 2, 8, 2, 128).transpose(0, 1, 2, 4, 3, 5).reshape(n, ROWS, 128)


def block_of(rows):
    n = rows.shape[0]
    return rows.reshape(n, 16, 2, 2, 8, 128).transpose(0, 1, 2, 4, 3, 5).reshape(n, 16, 16, 256)


def row(x, y, half):
    return x * 32 + (y // 8) * 16 + half * 8 + y % 8


def split(pair):
    high = pair.astype(BF16)
    return high, (pair - high.astype(F32)).astype(BF16)


def fold(square):
    return jnp.concatenate([square[8 * c : 8 * c + 8] for c in range(4)], axis=1)


def gram(left, right):
    full = lax.dot_general(left, right, (((1,), (1,)), ((), ())), preferred_element_type=F32)
    return full


def combine(full):
    return (full[32:, 32:] + full[32:, :32]) + full[:32, 32:] + full[:32, :32]


def main_kernel(b_hbm, r_hbm, o_hbm, g_ref, own_ref, st, w1, w2, rbuf, dbuf, p_ref, q_ref, acc, sem_in, sem_out, sem_r):
    def load_copy(k):
        return pltpu.make_async_copy(b_hbm.at[k], st.at[pl.ds(k * PITCH, ROWS)], sem_in.at[k])

    def store_copy(k):
        return pltpu.make_async_copy(st.at[pl.ds(k * PITCH, ROWS)], o_hbm.at[k], sem_out.at[k])

    rcopy = pltpu.make_async_copy(r_hbm, rbuf, sem_r)
    rcopy.start()
    for k in range(K):
        load_copy(k).start()
    rcopy.wait()

    @pl.loop(0, ROWS // 64)
    def _(i):
        part = pl.ds(pl.multiple_of(i * 64, 64), 64)
        center = 6.0 + rbuf[part, :]
        dbuf[part, :] = OMEGA / center
        rbuf[part, :] = 0.5 * center

    lane = lax.broadcasted_iota(jnp.int32, (8, 128), 1)
    first = lane == 0
    last = lane == 127
    zero = jnp.zeros((8, 128), F32)

    def z_sum(a, b):
        ra, rb = pltpu.roll(a, 1, 1), pltpu.roll(b, 1, 1)
        la, lb = pltpu.roll(a, 127, 1), pltpu.roll(b, 127, 1)
        return (
            jnp.where(first, zero, ra) + jnp.where(last, lb, la),
            jnp.where(first, ra, rb) + jnp.where(last, zero, lb),
        )

    def sweep(load, store):
        prev = None
        for x in range(0, 15):
            here = [None] * 16
            nxt = [None] * 16
            w = [None] * 15
            for y in range(0, 15):
                w[y] = [None, None]
                for h in range(2):
                    if x == 0 and y == 14:
                        continue
                    up = load(x, y + 1, h)
                    w[y][h] = up + load(x + 1, y, h)
                    here[y + 1] = here[y + 1] or [None, None]
                    here[y + 1][h] = up
                if x >= 1 and y >= 1:
                    c = here[y]
                    zs = z_sum(c[0], c[1])
                    for h in range(2):
                        s = (w[y][h] + prev[y - 1][h]) + zs[h]
                        d = dbuf[pl.ds(row(x, y, h), 8, stride=0), :]
                        store(x, y, h, (1.0 - OMEGA) * c[h] + d * s)
            prev = w

    @pl.loop(0, 4)
    def _(g):
        base = g * (8 * PITCH)

        @pl.loop(0, 8)
        def _(k):
            load_copy(g * 8 + k).wait()

        def stage(x, y, h):
            return pl.ds(base + row(x, y, h), 8, stride=PITCH)

        def work(x, y, h):
            return pl.ds(((x * 16 + y) * 2 + h) * 8, 8)

        def from_stage(x, y, h):
            return st[stage(x, y, h), :]

        def to_stage(x, y, h, v):
            st[stage(x, y, h), :] = v

        def reader(ref):
            return lambda x, y, h: ref[work(x, y, h), :]

        def writer(ref):
            def put(x, y, h, v):
                ref[work(x, y, h), :] = v

            return put

        for i in range(1, 15):
            for x, y in ((0, i), (15, i), (i, 0), (i, 15)):
                for h in range(2):
                    v = from_stage(x, y, h)
                    w1[work(x, y, h), :] = v
                    w2[work(x, y, h), :] = v
        sweep(from_stage, writer(w1))
        sweep(reader(w1), writer(w2))
        sweep(reader(w2), writer(w1))
        sweep(reader(w1), to_stage)

        @pl.loop(0, 8)
        def _(k):
            store_copy(g * 8 + k).start()

    def stage_pair(x, y, h, pair):
        at = x * 32 + ((y // 8) * 16 + h * 8 + y % 8)
        return [st[pl.ds(at + (2 * pair + o) * (8 * PITCH), 8, stride=PITCH), :] for o in range(2)]

    def halves(x, with_next):
        slot = lax.rem(x, 2)
        for pair in range(2):
            for h in range(2):
                pass
            up = [stage_pair(x, 0, h, pair) for h in range(2)]
            for y in range(16):
                c = up
                if y < 15:
                    up = [stage_pair(x, y + 1, h, pair) for h in range(2)]
                ahead = [stage_pair(x + 1, y, h, pair) for h in range(2)] if with_next else None
                q = [[None, None], [None, None]]
                for o in range(2):
                    a, b = c[0][o], c[1][o]
                    la, lb = pltpu.roll(a, 127, 1), pltpu.roll(b, 127, 1)
                    right = [jnp.where(last, lb, la), jnp.where(last, zero, lb)]
                    for h in range(2):
                        n = right[h]
                        if y < 15:
                            n = n + up[h][o]
                        if with_next:
                            n = n + ahead[h][o]
                        d = rbuf[pl.ds(x * 32 + ((y // 8) * 16 + h * 8 + y % 8), 8, stride=0), :]
                        q[h][o] = d * c[h][o] - n
                for h in range(2):
                    lanes = pl.ds(y * 256 + h * 128, 128)
                    hi, lo = split(jnp.concatenate(c[h], axis=0))
                    p_ref[slot, pl.ds(16 * pair, 16), lanes] = hi
                    p_ref[slot, pl.ds(32 + 16 * pair, 16), lanes] = lo
                    hi, lo = split(jnp.concatenate(q[h], axis=0))
                    q_ref[slot, pl.ds(16 * pair, 16), lanes] = hi
                    q_ref[slot, pl.ds(32 + 16 * pair, 16), lanes] = lo

    acc[...] = jnp.zeros_like(acc)
    halves(0, True)
    own_ref[0] = p_ref[0]

    @pl.loop(1, 15)
    def _(x):
        halves(x, True)
        slot = lax.rem(x - 1, 2)
        acc[...] += gram(p_ref[slot], q_ref[slot])

    halves(15, False)
    acc[...] += gram(p_ref[0], q_ref[0])
    acc[...] += gram(p_ref[1], q_ref[1])
    full = combine(acc[...])
    g_ref[...] = fold(full + full.T)

    for x in range(16):
        for pair in range(2):
            for h in range(2):
                hi, lo = split(jnp.concatenate(stage_pair(x, 0, h, pair), axis=0))
                lanes = pl.ds(x * 256 + h * 128, 128)
                own_ref[1, pl.ds(16 * pair, 16), lanes] = hi
                own_ref[1, pl.ds(32 + 16 * pair, 16), lanes] = lo

    for k in range(K):
        store_copy(k).wait()


def faces_kernel(b_hbm, x_ref, y_ref, sem):
    copies = [
        pltpu.make_async_copy(b_hbm.at[:, :, 1, :, pl.ds(7, 1), :], y_ref, sem.at[0]),
        pltpu.make_async_copy(b_hbm.at[:, 15], x_ref, sem.at[1]),
    ]
    for copy in copies:
        copy.start()
    for copy in copies:
        copy.wait()


def couple_kernel(copies, fx_hbm, fy_hbm, own_ref, g_ref, o_ref, sx, sy, p_ref, sem):
    def copy(which, ref, scratch, k):
        return pltpu.make_async_copy(ref.at[k], scratch.at[pl.ds(k * FPITCH, 32)], sem.at[which, k])

    sides = ((fx_hbm, sx), (fy_hbm, sy))
    for which, (ref, scratch) in enumerate(sides):
        for k in range(K):
            copy(which, ref, scratch, k).start()
    blocks = [g_ref[...]]
    for which, (ref, scratch) in enumerate(sides):
        for k in range(K):
            copy(which, ref, scratch, k).wait()
        for at in range(16):
            for h in range(2):
                line = row(0, at, h) if which == 0 else at * 2 + h
                for pair in range(2):
                    two = [scratch[pl.ds((2 * pair + o) * 8 * FPITCH + line, 8, stride=FPITCH), :] for o in range(2)]
                    hi, lo = split(jnp.concatenate(two, axis=0))
                    lanes = pl.ds(at * 256 + h * 128, 128)
                    p_ref[which, pl.ds(16 * pair, 16), lanes] = hi
                    p_ref[which, pl.ds(32 + 16 * pair, 16), lanes] = lo
        blocks.append(fold(-combine(gram(own_ref[which], p_ref[which]))))
    payload = jnp.concatenate(blocks, axis=0)
    for i in range(copies):
        o_ref[i] = payload


def finish_kernel(a_hbm, b_hbm, o_ref, a, b, m, t, sem):
    core = lax.rem(lax.axis_index("gy"), 2)
    for i, (src, dst) in enumerate(((a_hbm, a), (b_hbm, b))):
        pltpu.make_async_copy(src, dst, sem.at[i]).start()
    for i, (src, dst) in enumerate(((a_hbm, a), (b_hbm, b))):
        pltpu.make_async_copy(src, dst, sem.at[i]).wait()
    for block in range(3):
        for q in range(8):
            v = block * 8 + q
            for i, ref in enumerate((a, b)):
                c = core if i == 0 else 1 - core
                for j in range(8):
                    m[pl.ds(16 * j + c, 8, stride=2), :] = ref[pl.ds(v + 24 * 8 * j, 8, stride=24), :]
            turned = m[...].T
            for c in range(4):
                i = 8 * c + q
                part = turned[32 * c : 32 * c + 32]
                if block == 0:
                    o_ref[0, i] = part
                else:
                    o_ref[2 * block - 1, i] = part
                    t[pl.ds(i * 33, 32), :] = part
        if block:
            shift = 120 if block == 1 else 127
            for j in range(32):
                for i in range(4):
                    col = t[pl.ds(8 * i * 33 + j, 8, stride=33), :]
                    o_ref[2 * block, j, pl.ds(8 * i, 8), :] = pltpu.roll(col, shift, 1)


def on_device(basis, reaction):
    shape = jax.ShapeDtypeStruct
    rows = rows_of(basis)
    up_x, up_y = pl.pallas_call(
        faces_kernel,
        name="faces",
        out_shape=(shape((K, 2, 2, 8, 128), F32), shape((K, 16, 2, 1, 128), F32)),
        in_specs=[ANY],
        out_specs=(VM, VM),
        scratch_shapes=[pltpu.SemaphoreType.DMA((2,))],
    )(rows.reshape(K, 16, 2, 2, 8, 128))
    face_x = lax.ppermute(up_x.reshape(K, 32, 128), "gx", [(i, i + 1) for i in range(15)])
    face_y = lax.ppermute(up_y.reshape(K, 32, 128), "gy", [(i, i + 1) for i in range(7)])
    out, diag, own = pl.pallas_call(
        main_kernel,
        name="extend",
        out_shape=(shape((K, ROWS, 128), F32), shape((8, 128), F32), shape((2, 64, 4096), BF16)),
        in_specs=[ANY, ANY],
        out_specs=(ANY, VM, VM),
        scratch_shapes=[
            pltpu.VMEM((K * PITCH, 128), F32),
            pltpu.VMEM((4096, 128), F32),
            pltpu.VMEM((4096, 128), F32),
            pltpu.VMEM((ROWS, 128), F32),
            pltpu.VMEM((ROWS, 128), F32),
            pltpu.VMEM((2, 64, 4096), BF16),
            pltpu.VMEM((2, 64, 4096), BF16),
            pltpu.VMEM((64, 64), F32),
            pltpu.SemaphoreType.DMA((K,)),
            pltpu.SemaphoreType.DMA((K,)),
            pltpu.SemaphoreType.DMA,
        ],
        cost_estimate=pl.CostEstimate(flops=500_000_000, bytes_accessed=17_000_000, transcendentals=0),
    )(rows, rows_of(reaction[None])[0])
    payload = pl.pallas_call(
        functools.partial(couple_kernel, 64),
        name="couple",
        out_shape=shape((64, 24, 128), F32),
        in_specs=[ANY, ANY, VM, VM],
        out_specs=VM,
        scratch_shapes=[
            pltpu.VMEM((K * FPITCH, 128), F32),
            pltpu.VMEM((K * FPITCH, 128), F32),
            pltpu.VMEM((2, 64, 4096), BF16),
            pltpu.SemaphoreType.DMA((2, K)),
        ],
    )(face_x, face_y, own, diag)
    return out, payload


def finish(mine, other):
    shape = jax.ShapeDtypeStruct
    return pl.pallas_call(
        finish_kernel,
        name="finish",
        out_shape=shape((5, 32, 32, 128), F32),
        in_specs=[ANY, ANY],
        out_specs=VM,
        scratch_shapes=[
            pltpu.VMEM((64 * 24, 128), F32),
            pltpu.VMEM((64 * 24, 128), F32),
            pltpu.VMEM((128, 128), F32),
            pltpu.VMEM((32 * 33 + 7, 128), F32),
            pltpu.SemaphoreType.DMA((2,)),
        ],
    )(mine.reshape(64 * 24, 128), other.reshape(64 * 24, 128))


def solution(mesh):
    gx, gy = mesh.shape["gx"], mesh.shape["gy"]
    fine = Mesh(mesh.devices.reshape(gx, gy // 2, 2), ("gx", "gz", "core"))

    def local(basis, reaction):
        return on_device(basis, reaction)

    def exchange(payload):
        mine = lax.all_to_all(payload, ("gx", "gz"), 0, 0, tiled=True)
        return mine, lax.ppermute(mine, "core", [(0, 1), (1, 0)])

    def run(basis, reaction):
        rows, payload = jax.shard_map(
            local,
            mesh=mesh,
            in_specs=(P(None, "gx", "gy", None), P("gx", "gy", None)),
            out_specs=(P(("gx", "gy")), P(("gx", "gy"))),
            check_vma=False,
        )(basis, reaction)
        mine, other = jax.shard_map(
            exchange,
            mesh=fine,
            in_specs=P(("gx", "gz", "core")),
            out_specs=P(("gx", "gz", "core")),
            check_vma=False,
        )(payload)

        def last(rows, mine, other):
            return block_of(rows), finish(mine, other).transpose(3, 0, 1, 2)

        return jax.shard_map(
            last,
            mesh=mesh,
            in_specs=P(("gx", "gy")),
            out_specs=(P(None, "gx", "gy", None), P()),
            check_vma=False,
        )(rows, mine, other)

    return run
```

```python
import functools

import jax
import jax.numpy as jnp
from jax import lax
from jax.experimental import pallas as pl
from jax.experimental.pallas import tpu as pltpu
from jax.sharding import Mesh, PartitionSpec as P

K = 32
ROWS = 512
PITCH = 516
FPITCH = 36
OMEGA = 0.8
SWEEPS = 4
F32 = jnp.float32
BF16 = jnp.bfloat16
ANY = pl.BlockSpec(memory_space=pltpu.HBM)
VM = pl.BlockSpec(memory_space=pltpu.VMEM)


def rows_of(block):
    n = block.shape[0]
    return block.reshape(n, 16, 2, 8, 2, 128).transpose(0, 1, 2, 4, 3, 5).reshape(n, ROWS, 128)


def block_of(rows):
    n = rows.shape[0]
    return rows.reshape(n, 16, 2, 2, 8, 128).transpose(0, 1, 2, 4, 3, 5).reshape(n, 16, 16, 256)


def row(x, y, half):
    return x * 32 + (y // 8) * 16 + half * 8 + y % 8


def split(pair):
    high = pair.astype(BF16)
    return high, (pair - high.astype(F32)).astype(BF16)


def fold(square):
    return jnp.concatenate([square[8 * c : 8 * c + 8] for c in range(4)], axis=1)


def put(ref, line, pair, two):
    high, low = split(jnp.concatenate(two, axis=0))
    ref[line, pl.ds(16 * pair, 16), :] = high
    ref[line, pl.ds(32 + 16 * pair, 16), :] = low


def gram(left, right):
    left = jnp.concatenate([left[i] for i in range(32)], axis=1)
    right = jnp.concatenate([right[i] for i in range(32)], axis=1)
    return lax.dot_general(left, right, (((1,), (1,)), ((), ())), preferred_element_type=F32)


def combine(full):
    return (full[32:, 32:] + full[32:, :32]) + full[:32, 32:] + full[:32, :32]


def main_kernel(b_hbm, r_ref, o_hbm, g_ref, own_ref, st, w1, w2, rbuf, dbuf, pa, qa, pb, qb, acc, sem_in, sem_out):
    def load_copy(k):
        return pltpu.make_async_copy(b_hbm.at[k], st.at[pl.ds(k * PITCH, ROWS)], sem_in.at[k])

    def store_copy(k):
        return pltpu.make_async_copy(st.at[pl.ds(k * PITCH, ROWS)], o_hbm.at[k], sem_out.at[k])

    for k in range(K):
        load_copy(k).start()

    @pl.loop(0, ROWS // 64)
    def _(i):
        part = pl.ds(pl.multiple_of(i * 64, 64), 64)
        center = 6.0 + r_ref[part, :]
        dbuf[part, :] = OMEGA / center
        rbuf[part, :] = 0.5 * center

    lane = lax.broadcasted_iota(jnp.int32, (8, 128), 1)
    first = lane == 0
    last = lane == 127
    zero = jnp.zeros((8, 128), F32)

    def z_sum(a, b):
        ra, rb = pltpu.roll(a, 1, 1), pltpu.roll(b, 1, 1)
        la, lb = pltpu.roll(a, 127, 1), pltpu.roll(b, 127, 1)
        return (
            jnp.where(first, zero, ra) + jnp.where(last, lb, la),
            jnp.where(first, ra, rb) + jnp.where(last, zero, lb),
        )

    def sweep(load, store):
        starts = [(0, j) for j in range(13, -1, -1)] + [(i, 0) for i in range(1, 14)]
        for x, y in starts:
            before = None
            while x <= 14 and y <= 14:
                ahead = [load(x, y + 1, h) + load(x + 1, y, h) for h in range(2)]
                if before is not None:
                    c = [load(x, y, h) for h in range(2)]
                    beside = z_sum(c[0], c[1])
                    for h in range(2):
                        total = (ahead[h] + before[h]) + beside[h]
                        d = dbuf[pl.ds(row(x, y, h), 8, stride=0), :]
                        store(x, y, h, (1.0 - OMEGA) * c[h] + d * total)
                before = ahead
                x, y = x + 1, y + 1

    @pl.loop(0, 4)
    def _(g):
        base = g * (8 * PITCH)

        @pl.loop(0, 8)
        def _(k):
            load_copy(g * 8 + k).wait()

        def stage(x, y, h):
            return pl.ds(base + row(x, y, h), 8, stride=PITCH)

        def work(x, y, h):
            return pl.ds(((x * 16 + y) * 2 + h) * 8, 8)

        def from_stage(x, y, h):
            return st[stage(x, y, h), :]

        def to_stage(x, y, h, v):
            st[stage(x, y, h), :] = v

        def reader(ref):
            return lambda x, y, h: ref[work(x, y, h), :]

        def writer(ref):
            def put(x, y, h, v):
                ref[work(x, y, h), :] = v

            return put

        for i in range(1, 15):
            for x, y in ((0, i), (15, i), (i, 0), (i, 15)):
                for h in range(2):
                    v = from_stage(x, y, h)
                    w1[work(x, y, h), :] = v
                    w2[work(x, y, h), :] = v
        sweep(from_stage, writer(w1))
        sweep(reader(w1), writer(w2))
        sweep(reader(w2), writer(w1))
        sweep(reader(w1), to_stage)

        @pl.loop(0, 8)
        def _(k):
            store_copy(g * 8 + k).start()

    def stage_pair(x, y, h, pair):
        at = x * 32 + ((y // 8) * 16 + h * 8 + y % 8)
        return [st[pl.ds(at + (2 * pair + o) * (8 * PITCH), 8, stride=PITCH), :] for o in range(2)]

    def halves(x, p_ref, q_ref, with_next=True):
        for pair in range(2):
            up = [stage_pair(x, 0, h, pair) for h in range(2)]
            for y in range(16):
                c = up
                if y < 15:
                    up = [stage_pair(x, y + 1, h, pair) for h in range(2)]
                ahead = [stage_pair(x + 1, y, h, pair) for h in range(2)] if with_next else None
                q = [[None, None], [None, None]]
                for o in range(2):
                    a, b = c[0][o], c[1][o]
                    la, lb = pltpu.roll(a, 127, 1), pltpu.roll(b, 127, 1)
                    right = [jnp.where(last, lb, la), jnp.where(last, zero, lb)]
                    for h in range(2):
                        n = right[h]
                        if y < 15:
                            n = n + up[h][o]
                        if with_next:
                            n = n + ahead[h][o]
                        d = rbuf[pl.ds(x * 32 + ((y // 8) * 16 + h * 8 + y % 8), 8, stride=0), :]
                        q[h][o] = d * c[h][o] - n
                for h in range(2):
                    put(p_ref, 2 * y + h, pair, c[h])
                    put(q_ref, 2 * y + h, pair, q[h])

    halves(0, pa, qa)
    own_ref[0] = pa[...]
    acc[...] = jnp.zeros_like(acc)

    @pl.loop(0, 7)
    def _(i):
        first_gram = gram(pa, qa)
        halves(2 * i + 1, pb, qb)
        second_gram = gram(pb, qb)
        halves(2 * i + 2, pa, qa)
        acc[...] += first_gram + second_gram

    first_gram = gram(pa, qa)
    halves(15, pb, qb, False)
    acc[...] += first_gram + gram(pb, qb)
    full = combine(acc[...])
    g_ref[...] = fold(full + full.T)

    for x in range(16):
        for pair in range(2):
            for h in range(2):
                put(own_ref.at[1], 2 * x + h, pair, stage_pair(x, 0, h, pair))

    for k in range(K):
        store_copy(k).wait()


def faces_kernel(b_hbm, rows_hbm, x_ref, y_ref, sem, sem_x):
    copies = [pltpu.make_async_copy(b_hbm.at[:, :, 1, :, pl.ds(7, 1), :], y_ref.at[:, pl.ds(0, 16)], sem)]
    for k in range(K):
        part = x_ref.at[pl.ds(k * FPITCH, 32)]
        copies.append(pltpu.make_async_copy(rows_hbm.at[k, pl.ds(480, 32)], part, sem_x.at[k]))
    for copy in copies:
        copy.start()
    for copy in copies:
        copy.wait()


def couple_kernel(copies, fx_ref, fy_ref, own_ref, g_ref, o_ref, p_ref):
    blocks = [g_ref[...]]
    for which, face in enumerate((fx_ref, fy_ref)):
        for at in range(16):
            for h in range(2):
                line = row(0, at, h) if which == 0 else at * 2 + h
                for pair in range(2):
                    two = [face[pl.ds((2 * pair + o) * 8 * FPITCH + line, 8, stride=FPITCH), :] for o in range(2)]
                    put(p_ref.at[which], 2 * at + h, pair, two)
        blocks.append(fold(-combine(gram(own_ref.at[which], p_ref.at[which]))))
    payload = jnp.concatenate(blocks, axis=0)
    for i in range(copies):
        o_ref[i] = payload


def finish_kernel(a, b, o_hbm, o_ref, m, t, sem):
    core = lax.rem(lax.axis_index("gy"), 2)

    def leave(block):
        return pltpu.make_async_copy(o_ref.at[block], o_hbm.at[block], sem.at[block])

    for block in range(3):
        for q in range(8):
            v = block * 8 + q
            for i, ref in enumerate((a, b)):
                c = core if i == 0 else 1 - core
                for j in range(8):
                    m[pl.ds(16 * j + c, 8, stride=2), :] = ref[pl.ds(v + 24 * 8 * j, 8, stride=24), :]
            turned = m[...].T
            for c in range(4):
                i = 8 * c + q
                part = turned[32 * c : 32 * c + 32]
                if block == 0:
                    o_ref[0, i] = part
                else:
                    o_ref[2 * block - 1, i] = part
                    t[pl.ds(i * 33, 32), :] = part
        if block:
            shift = 120 if block == 1 else 127
            for j in range(32):
                for i in range(4):
                    col = t[pl.ds(8 * i * 33 + j, 8, stride=33), :]
                    o_ref[2 * block, j, pl.ds(8 * i, 8), :] = pltpu.roll(col, shift, 1)
            leave(2 * block - 1).start()
            leave(2 * block).start()
        else:
            leave(0).start()
    for block in range(5):
        leave(block).wait()


def extend_call(rows, reaction):
    shape = jax.ShapeDtypeStruct
    return pl.pallas_call(
        main_kernel,
        name="extend",
        compiler_params=pltpu.CompilerParams(vmem_limit_bytes=57 << 20),
        out_shape=(shape((K, ROWS, 128), F32), shape((8, 128), F32), shape((2, 32, 64, 128), BF16)),
        in_specs=[ANY, VM],
        out_specs=(ANY, VM, VM),
        scratch_shapes=[
            pltpu.VMEM((K * PITCH, 128), F32),
            pltpu.VMEM((4096, 128), F32),
            pltpu.VMEM((4096, 128), F32),
            pltpu.VMEM((ROWS, 128), F32),
            pltpu.VMEM((ROWS, 128), F32),
            pltpu.VMEM((32, 64, 128), BF16),
            pltpu.VMEM((32, 64, 128), BF16),
            pltpu.VMEM((32, 64, 128), BF16),
            pltpu.VMEM((32, 64, 128), BF16),
            pltpu.VMEM((64, 64), F32),
            pltpu.SemaphoreType.DMA((K,)),
            pltpu.SemaphoreType.DMA((K,)),
        ],
        cost_estimate=pl.CostEstimate(flops=500_000_000, bytes_accessed=17_000_000, transcendentals=0),
    )(rows, reaction)


def on_device(basis, reaction):
    shape = jax.ShapeDtypeStruct
    rows = rows_of(basis)
    up_x, up_y = pl.pallas_call(
        faces_kernel,
        name="faces",
        compiler_params=pltpu.CompilerParams(vmem_limit_bytes=54 << 20),
        out_shape=(shape((K * FPITCH, 128), F32), shape((K, FPITCH // 2, 2, 1, 128), F32)),
        in_specs=[ANY, ANY],
        out_specs=(VM, VM),
        scratch_shapes=[pltpu.SemaphoreType.DMA, pltpu.SemaphoreType.DMA((K,))],
    )(rows.reshape(K, 16, 2, 2, 8, 128), rows)
    face_x = lax.ppermute(up_x, "gx", [(i, i + 1) for i in range(15)])
    face_y = lax.ppermute(up_y.reshape(K * FPITCH, 128), "gy", [(i, i + 1) for i in range(7)])
    out, diag, own = extend_call(rows, rows_of(reaction[None])[0])
    payload = pl.pallas_call(
        functools.partial(couple_kernel, 64),
        name="couple",
        compiler_params=pltpu.CompilerParams(vmem_limit_bytes=12 << 20),
        out_shape=shape((64, 24, 128), F32),
        in_specs=[VM, VM, VM, VM],
        out_specs=VM,
        scratch_shapes=[pltpu.VMEM((2, 32, 64, 128), BF16)],
    )(face_x, face_y, own, diag)
    return out, payload


def finish(mine, other):
    shape = jax.ShapeDtypeStruct
    return pl.pallas_call(
        finish_kernel,
        name="finish",
        compiler_params=pltpu.CompilerParams(vmem_limit_bytes=12 << 20),
        out_shape=shape((5, 32, 32, 128), F32),
        in_specs=[VM, VM],
        out_specs=ANY,
        scratch_shapes=[
            pltpu.VMEM((5, 32, 32, 128), F32),
            pltpu.VMEM((128, 128), F32),
            pltpu.VMEM((32 * 33 + 7, 128), F32),
            pltpu.SemaphoreType.DMA((5,)),
        ],
    )(mine.reshape(64 * 24, 128), other.reshape(64 * 24, 128))


def solution(mesh):
    gx, gy = mesh.shape["gx"], mesh.shape["gy"]
    fine = Mesh(mesh.devices.reshape(gx, gy // 2, 2), ("gx", "gz", "core"))

    def local(basis, reaction):
        return on_device(basis, reaction)

    def exchange(payload):
        mine = lax.all_to_all(payload, ("gx", "gz"), 0, 0, tiled=True)
        return mine, lax.ppermute(mine, "core", [(0, 1), (1, 0)])

    def run(basis, reaction):
        rows, payload = jax.shard_map(
            local,
            mesh=mesh,
            in_specs=(P(None, "gx", "gy", None), P("gx", "gy", None)),
            out_specs=(P(("gx", "gy")), P(("gx", "gy"))),
            check_vma=False,
        )(basis, reaction)
        mine, other = jax.shard_map(
            exchange,
            mesh=fine,
            in_specs=P(("gx", "gz", "core")),
            out_specs=P(("gx", "gz", "core")),
            check_vma=False,
        )(payload)

        def last(rows, mine, other):
            return block_of(rows), finish(mine, other).transpose(3, 0, 1, 2)

        return jax.shard_map(
            last,
            mesh=mesh,
            in_specs=P(("gx", "gy")),
            out_specs=(P(None, "gx", "gy", None), P()),
            check_vma=False,
        )(rows, mine, other)

    return run
```

```python
import functools

import jax
import jax.numpy as jnp
from jax import lax
from jax.experimental import pallas as pl
from jax.experimental.pallas import tpu as pltpu
from jax.sharding import Mesh, PartitionSpec as P

K = 32
ROWS = 512
PITCH = 516
FPITCH = 36
OMEGA = 0.8
SWEEPS = 4
F32 = jnp.float32
BF16 = jnp.bfloat16
ANY = pl.BlockSpec(memory_space=pltpu.HBM)
VM = pl.BlockSpec(memory_space=pltpu.VMEM)


STARTS = [(0, j) for j in range(13, -1, -1)] + [(i, 0) for i in range(1, 14)]
ROTATED_STARTS = [p for p in STARTS if abs(p[0] - p[1]) < 5]
LINED_STARTS = [p for p in STARTS if p not in ROTATED_STARTS]
LINED = [(x + i, y + i) for x, y in LINED_STARTS for i in range(1, 15 - max(x, y))]


def rows_of(block):
    n = block.shape[0]
    return block.reshape(n, 16, 2, 8, 2, 128).transpose(0, 1, 2, 4, 3, 5).reshape(n, ROWS, 128)


def block_of(rows):
    n = rows.shape[0]
    return rows.reshape(n, 16, 2, 2, 8, 128).transpose(0, 1, 2, 4, 3, 5).reshape(n, 16, 16, 256)


def row(x, y, half):
    return x * 32 + (y // 8) * 16 + half * 8 + y % 8


def split(pair):
    high = pair.astype(BF16)
    return high, (pair - high.astype(F32)).astype(BF16)


def fold(square):
    return jnp.concatenate([square[8 * c : 8 * c + 8] for c in range(4)], axis=1)


def put(ref, line, pair, two):
    high, low = split(jnp.concatenate(two, axis=0))
    ref[line, pl.ds(16 * pair, 16), :] = high
    ref[line, pl.ds(32 + 16 * pair, 16), :] = low


def gram(left, right):
    left = jnp.concatenate([left[i] for i in range(32)], axis=1)
    right = jnp.concatenate([right[i] for i in range(32)], axis=1)
    return lax.dot_general(left, right, (((1,), (1,)), ((), ())), preferred_element_type=F32)


def combine(full):
    return (full[32:, 32:] + full[32:, :32]) + full[:32, 32:] + full[:32, :32]


def main_kernel(b_hbm, r_hbm, o_hbm, g_ref, own_hbm, own_ref, st, w1, w2, rbuf, dbuf, pa, qa, pb, qb, acc, z_in, z_out, tri, sem_in, sem_out, sem_r, sem_own):
    def load_copy(k):
        return pltpu.make_async_copy(b_hbm.at[k], st.at[pl.ds(k * PITCH, ROWS)], sem_in.at[k])

    def store_copy(k):
        return pltpu.make_async_copy(st.at[pl.ds(k * PITCH, ROWS)], o_hbm.at[k], sem_out.at[k])

    reaction = pltpu.make_async_copy(r_hbm, rbuf, sem_r)
    reaction.start()
    for k in range(K):
        load_copy(k).start()

    apart = lax.broadcasted_iota(jnp.int32, (256, 256), 0) - lax.broadcasted_iota(jnp.int32, (256, 256), 1)
    band = jnp.where(jnp.abs(apart) == 1, 1.0, 0.0).astype(BF16)
    tri[pl.ds(0, 256), :] = band
    tri[pl.ds(256, 256), :] = band

    reaction.wait()

    @pl.loop(0, ROWS // 64)
    def _(i):
        part = pl.ds(pl.multiple_of(i * 64, 64), 64)
        center = 6.0 + rbuf[part, :]
        dbuf[part, :] = OMEGA / center
        rbuf[part, :] = 0.5 * center

    lane = lax.broadcasted_iota(jnp.int32, (8, 128), 1)
    first = lane == 0
    last = lane == 127
    zero = jnp.zeros((8, 128), F32)

    def z_sum(a, b):
        ra, rb = pltpu.roll(a, 1, 1), pltpu.roll(b, 1, 1)
        la, lb = pltpu.roll(a, 127, 1), pltpu.roll(b, 127, 1)
        return (
            jnp.where(first, zero, ra) + jnp.where(last, lb, la),
            jnp.where(first, ra, rb) + jnp.where(last, zero, lb),
        )

    def sweep(load, store):
        for j in range(0, len(LINED), 2):
            for h in range(2):
                high, low = split(jnp.concatenate([load(*LINED[j], h), load(*LINED[j + 1], h)], axis=0))
                z_in[h, pl.ds(8 * j, 16), :] = high
                z_in[2 + h, pl.ds(8 * j, 16), :] = low
        parts = jnp.concatenate([z_in[i] for i in range(4)], axis=1)
        sums = lax.dot_general(parts, tri[...], (((1,), (0,)), ((), ())), preferred_element_type=F32)
        for h in range(2):
            z_out[h] = sums[:, 128 * h : 128 * h + 128]
        for x, y in ROTATED_STARTS + LINED_STARTS:
            lined = (x, y) in LINED_STARTS
            before = None
            while x <= 14 and y <= 14:
                ahead = [load(x, y + 1, h) + load(x + 1, y, h) for h in range(2)]
                if before is not None:
                    c = [load(x, y, h) for h in range(2)]
                    if lined:
                        at = pl.ds(8 * LINED.index((x, y)), 8)
                        beside = [z_out[h, at, :] for h in range(2)]
                    else:
                        beside = z_sum(c[0], c[1])
                    for h in range(2):
                        total = (ahead[h] + before[h]) + beside[h]
                        d = dbuf[pl.ds(row(x, y, h), 8, stride=0), :]
                        store(x, y, h, (1.0 - OMEGA) * c[h] + d * total)
                before = ahead
                x, y = x + 1, y + 1

    @pl.loop(0, 4)
    def _(g):
        base = g * (8 * PITCH)

        @pl.loop(0, 8)
        def _(k):
            load_copy(g * 8 + k).wait()

        def stage(x, y, h):
            return pl.ds(base + row(x, y, h), 8, stride=PITCH)

        def work(x, y, h):
            return pl.ds(((x * 16 + y) * 2 + h) * 8, 8)

        def from_stage(x, y, h):
            return st[stage(x, y, h), :]

        def to_stage(x, y, h, v):
            st[stage(x, y, h), :] = v

        def reader(ref):
            return lambda x, y, h: ref[work(x, y, h), :]

        def writer(ref):
            def put(x, y, h, v):
                ref[work(x, y, h), :] = v

            return put

        for i in range(1, 15):
            for x, y in ((0, i), (15, i), (i, 0), (i, 15)):
                for h in range(2):
                    v = from_stage(x, y, h)
                    w1[work(x, y, h), :] = v
                    w2[work(x, y, h), :] = v
        sweep(from_stage, writer(w1))
        sweep(reader(w1), writer(w2))
        sweep(reader(w2), writer(w1))
        sweep(reader(w1), to_stage)

        @pl.loop(0, 8)
        def _(k):
            store_copy(g * 8 + k).start()

    def stage_pair(x, y, h, pair):
        at = x * 32 + ((y // 8) * 16 + h * 8 + y % 8)
        return [st[pl.ds(at + (2 * pair + o) * (8 * PITCH), 8, stride=PITCH), :] for o in range(2)]

    def halves(x, p_ref, q_ref, with_next=True):
        for pair in range(2):
            up = [stage_pair(x, 0, h, pair) for h in range(2)]
            for y in range(16):
                c = up
                if y < 15:
                    up = [stage_pair(x, y + 1, h, pair) for h in range(2)]
                ahead = [stage_pair(x + 1, y, h, pair) for h in range(2)] if with_next else None
                q = [[None, None], [None, None]]
                for o in range(2):
                    a, b = c[0][o], c[1][o]
                    la, lb = pltpu.roll(a, 127, 1), pltpu.roll(b, 127, 1)
                    right = [jnp.where(last, lb, la), jnp.where(last, zero, lb)]
                    for h in range(2):
                        n = right[h]
                        if y < 15:
                            n = n + up[h][o]
                        if with_next:
                            n = n + ahead[h][o]
                        d = rbuf[pl.ds(x * 32 + ((y // 8) * 16 + h * 8 + y % 8), 8, stride=0), :]
                        q[h][o] = d * c[h][o] - n
                for h in range(2):
                    put(p_ref, 2 * y + h, pair, c[h])
                    put(q_ref, 2 * y + h, pair, q[h])

    halves(0, pa, qa)
    own_ref[0] = pa[...]
    leave_x = pltpu.make_async_copy(own_ref.at[0], own_hbm.at[0], sem_own.at[0])
    leave_y = pltpu.make_async_copy(own_ref.at[1], own_hbm.at[1], sem_own.at[1])
    leave_x.start()
    acc[...] = jnp.zeros_like(acc)

    @pl.loop(0, 7)
    def _(i):
        first_gram = gram(pa, qa)
        halves(2 * i + 1, pb, qb)
        second_gram = gram(pb, qb)
        halves(2 * i + 2, pa, qa)
        acc[...] += first_gram + second_gram

    first_gram = gram(pa, qa)
    halves(15, pb, qb, False)
    for x in range(16):
        for pair in range(2):
            for h in range(2):
                put(own_ref.at[1], 2 * x + h, pair, stage_pair(x, 0, h, pair))
    leave_y.start()
    acc[...] += first_gram + gram(pb, qb)
    full = combine(acc[...])
    g_ref[...] = fold(full + full.T)

    leave_x.wait()
    leave_y.wait()
    for k in range(K):
        store_copy(k).wait()


def faces_kernel(b_hbm, rows_hbm, x_ref, y_ref, sem, sem_x):
    copies = [pltpu.make_async_copy(b_hbm.at[:, :, 1, :, pl.ds(7, 1), :], y_ref.at[:, pl.ds(0, 16)], sem)]
    for k in range(K):
        part = x_ref.at[pl.ds(k * FPITCH, 32)]
        copies.append(pltpu.make_async_copy(rows_hbm.at[k, pl.ds(480, 32)], part, sem_x.at[k]))
    for copy in copies:
        copy.start()
    for copy in copies:
        copy.wait()


def couple_kernel(copies, fx_ref, fy_ref, own_hbm, g_hbm, o_ref, p_ref, own_ref, g_ref, sem):
    get = [
        pltpu.make_async_copy(g_hbm, g_ref, sem.at[0]),
        pltpu.make_async_copy(own_hbm, own_ref, sem.at[1]),
    ]
    for copy in get:
        copy.start()
    for which, face in enumerate((fx_ref, fy_ref)):
        for at in range(16):
            for h in range(2):
                line = row(0, at, h) if which == 0 else at * 2 + h
                for pair in range(2):
                    two = [face[pl.ds((2 * pair + o) * 8 * FPITCH + line, 8, stride=FPITCH), :] for o in range(2)]
                    put(p_ref.at[which], 2 * at + h, pair, two)
    for copy in get:
        copy.wait()
    blocks = [g_ref[...]]
    for which in range(2):
        blocks.append(fold(-combine(gram(own_ref.at[which], p_ref.at[which]))))
    payload = jnp.concatenate(blocks, axis=0)
    for i in range(copies):
        o_ref[i] = payload


def finish_kernel(a, b, o_hbm, o_ref, m, t, sem):
    core = lax.rem(lax.axis_index("gy"), 2)

    def leave(block):
        return pltpu.make_async_copy(o_ref.at[block], o_hbm.at[block], sem.at[block])

    for block in range(3):
        for q in range(8):
            v = block * 8 + q
            for i, ref in enumerate((a, b)):
                c = core if i == 0 else 1 - core
                for j in range(8):
                    m[pl.ds(16 * j + c, 8, stride=2), :] = ref[pl.ds(v + 24 * 8 * j, 8, stride=24), :]
            turned = m[...].T
            for c in range(4):
                i = 8 * c + q
                part = turned[32 * c : 32 * c + 32]
                if block == 0:
                    o_ref[0, i] = part
                else:
                    o_ref[2 * block - 1, i] = part
                    t[pl.ds(i * 33, 32), :] = part
        if block:
            shift = 120 if block == 1 else 127
            for j in range(32):
                for i in range(4):
                    col = t[pl.ds(8 * i * 33 + j, 8, stride=33), :]
                    o_ref[2 * block, j, pl.ds(8 * i, 8), :] = pltpu.roll(col, shift, 1)
            leave(2 * block - 1).start()
            leave(2 * block).start()
        else:
            leave(0).start()
    for block in range(5):
        leave(block).wait()


def extend_call(rows, reaction):
    shape = jax.ShapeDtypeStruct
    return pl.pallas_call(
        main_kernel,
        name="extend",
        compiler_params=pltpu.CompilerParams(vmem_limit_bytes=46 << 20),
        out_shape=(shape((K, ROWS, 128), F32), shape((8, 128), F32), shape((2, 32, 64, 128), BF16)),
        in_specs=[ANY, ANY],
        out_specs=(ANY, VM, ANY),
        scratch_shapes=[
            pltpu.VMEM((2, 32, 64, 128), BF16),
            pltpu.VMEM((K * PITCH, 128), F32),
            pltpu.VMEM((4096, 128), F32),
            pltpu.VMEM((4096, 128), F32),
            pltpu.VMEM((ROWS, 128), F32),
            pltpu.VMEM((ROWS, 128), F32),
            pltpu.VMEM((32, 64, 128), BF16),
            pltpu.VMEM((32, 64, 128), BF16),
            pltpu.VMEM((32, 64, 128), BF16),
            pltpu.VMEM((32, 64, 128), BF16),
            pltpu.VMEM((64, 64), F32),
            pltpu.VMEM((4, 8 * len(LINED), 128), BF16),
            pltpu.VMEM((2, 8 * len(LINED), 128), F32),
            pltpu.VMEM((512, 256), BF16),
            pltpu.SemaphoreType.DMA((K,)),
            pltpu.SemaphoreType.DMA((K,)),
            pltpu.SemaphoreType.DMA,
            pltpu.SemaphoreType.DMA((2,)),
        ],
        cost_estimate=pl.CostEstimate(flops=500_000_000, bytes_accessed=17_000_000, transcendentals=0),
    )(rows, reaction)


def on_device(basis, reaction):
    shape = jax.ShapeDtypeStruct
    rows = rows_of(basis)
    up_x, up_y = pl.pallas_call(
        faces_kernel,
        name="faces",
        compiler_params=pltpu.CompilerParams(vmem_limit_bytes=54 << 20),
        out_shape=(shape((K * FPITCH, 128), F32), shape((K, FPITCH // 2, 2, 1, 128), F32)),
        in_specs=[ANY, ANY],
        out_specs=(VM, VM),
        scratch_shapes=[pltpu.SemaphoreType.DMA, pltpu.SemaphoreType.DMA((K,))],
    )(rows.reshape(K, 16, 2, 2, 8, 128), rows)
    face_x = lax.ppermute(up_x, "gx", [(i, i + 1) for i in range(15)])
    face_y = lax.ppermute(up_y.reshape(K * FPITCH, 128), "gy", [(i, i + 1) for i in range(7)])
    out, diag, own = extend_call(rows, rows_of(reaction[None])[0])
    payload = pl.pallas_call(
        functools.partial(couple_kernel, 64),
        name="couple",
        compiler_params=pltpu.CompilerParams(vmem_limit_bytes=12 << 20),
        out_shape=shape((64, 24, 128), F32),
        in_specs=[VM, VM, ANY, ANY],
        out_specs=VM,
        scratch_shapes=[
            pltpu.VMEM((2, 32, 64, 128), BF16),
            pltpu.VMEM((2, 32, 64, 128), BF16),
            pltpu.VMEM((8, 128), F32),
            pltpu.SemaphoreType.DMA((2,)),
        ],
    )(face_x, face_y, own, diag)
    return out, payload


def finish(mine, other):
    shape = jax.ShapeDtypeStruct
    return pl.pallas_call(
        finish_kernel,
        name="finish",
        compiler_params=pltpu.CompilerParams(vmem_limit_bytes=12 << 20),
        out_shape=shape((5, 32, 32, 128), F32),
        in_specs=[VM, VM],
        out_specs=ANY,
        scratch_shapes=[
            pltpu.VMEM((5, 32, 32, 128), F32),
            pltpu.VMEM((128, 128), F32),
            pltpu.VMEM((32 * 33 + 7, 128), F32),
            pltpu.SemaphoreType.DMA((5,)),
        ],
    )(mine.reshape(64 * 24, 128), other.reshape(64 * 24, 128))


def solution(mesh):
    gx, gy = mesh.shape["gx"], mesh.shape["gy"]
    fine = Mesh(mesh.devices.reshape(gx, gy // 2, 2), ("gx", "gz", "core"))

    def local(basis, reaction):
        return on_device(basis, reaction)

    def exchange(payload):
        mine = lax.all_to_all(payload, ("gx", "gz"), 0, 0, tiled=True)
        return mine, lax.ppermute(mine, "core", [(0, 1), (1, 0)])

    def run(basis, reaction):
        rows, payload = jax.shard_map(
            local,
            mesh=mesh,
            in_specs=(P(None, "gx", "gy", None), P("gx", "gy", None)),
            out_specs=(P(("gx", "gy")), P(("gx", "gy"))),
            check_vma=False,
        )(basis, reaction)
        mine, other = jax.shard_map(
            exchange,
            mesh=fine,
            in_specs=P(("gx", "gz", "core")),
            out_specs=P(("gx", "gz", "core")),
            check_vma=False,
        )(payload)

        def last(rows, mine, other):
            return block_of(rows), finish(mine, other).transpose(3, 0, 1, 2)

        return jax.shard_map(
            last,
            mesh=mesh,
            in_specs=P(("gx", "gy")),
            out_specs=(P(None, "gx", "gy", None), P()),
            check_vma=False,
        )(rows, mine, other)

    return run
```
